32 devices in a mesh: mem: 8 (over z, x), grid: 4 (over y, core).
Axes of the slice: x: 2, y: 2, z: 4, core: 2. Of those that a mesh axis runs over, the one named last changes fastest.
Arguments:
- alpha: bfloat16 [16, 8, 768, 1536], P('mem', None, 'grid'), may hold values from -6 to 6
- perturbation: bfloat16 [16, 8, 768, 1536], P('mem', None, 'grid'), may hold values from -6 to 6
- legendre: bfloat16 [192, 128, 768], P('grid'), may hold values from -0.21875 to 0.21875
- response: float32 [192, 128], P('grid'), may hold values from 0.2 to 2
Outputs:
- increment: float32 [8, 768, 1536], P('mem', 'grid')
The draws below stay inside these ranges and needn't reach their ends.
All inputs are finite; a program needn't handle non-finite values.
Results may differ from the reference program's by a relative error of at most 0.0063.
Values may be sent and summed in bfloat16 or wider, within the bound.
A program may use at most 128 MiB of HBM per device.

```python
import math
import jax
import jax.numpy as jnp
from jax import lax

NLON = 1536
NLAT = 768
KEEP = 192
NN = 128
MEMBERS = 16
LEV = 8


def block_scale(stream_key, extent, split, least, top_value):
    def one(axis_at, blocks):
        heights = jax.random.uniform(jax.random.fold_in(jax.random.fold_in(stream_key, 6), axis_at), (blocks,), jnp.float32, least / len(split), top_value / len(split))
        return jnp.repeat(jnp.exp(heights), extent[axis_at] // blocks).reshape((-1,) + (1,) * (len(extent) - axis_at - 1))

    level = one(*split[0])
    for cut in split[1:]:
        level = level * one(*cut)
    return level


def gaussian(stream_key, extent, deviation, most, pieces=(), kind=jnp.bfloat16):
    result = deviation * jax.random.normal(stream_key, extent, jnp.float32)
    if pieces:
        result = result * block_scale(stream_key, extent, pieces, -0.22, 0.18)
    return jnp.clip(result, -most, most).astype(kind)


def setup_inputs(seed: int = 0) -> dict:
    streams_of = jax.random.split(jax.random.key(seed), 5)
    return {
        "alpha": gaussian(streams_of[0], (MEMBERS, LEV, NLAT, NLON), 1.0, 6.0, ((0, 8), (2, 4))),
        "perturbation": gaussian(streams_of[1], (MEMBERS, LEV, NLAT, NLON), 1.0, 6.0, ((0, 8), (2, 4))),
        "legendre": gaussian(streams_of[2], (KEEP, NN, NLAT), NLAT ** -0.5, 0.21875, ((0, 4),)),
        "response": jnp.clip(jnp.exp(math.log(2.0) - 2.3025851 * jax.random.uniform(streams_of[3], (KEEP, NN), jnp.float32) ** block_scale(streams_of[3], (KEEP, NN), ((0, 4),), -0.2, 0.2)), 0.2, 2.0),
    }


def build_tables(lon_count, keep):
    col = jnp.arange(2 * keep, dtype=jnp.int32)
    part = col // keep
    wave = col % keep
    lon = jnp.arange(lon_count, dtype=jnp.int32)
    phase = lon[:, None] * wave[None, :] % lon_count
    angle = phase.astype(jnp.float32) * jnp.float32(2.0 * math.pi / lon_count)
    basis = jnp.where(part[None, :] == 0, jnp.cos(angle), jnp.sin(angle))
    weight = jnp.where(wave == 0, jnp.float32(1.0), jnp.float32(2.0)) / jnp.float32(lon_count)
    forward = basis.astype(jnp.bfloat16)
    inverse = jnp.transpose(basis * weight[None, :]).astype(jnp.bfloat16)
    return (forward, inverse)

def reference(alpha, perturbation, legendre, response):
    members = alpha.shape[0]
    forward, inverse = build_tables(NLON, KEEP)
    legendre_wide = legendre.astype(jnp.float32)

    def one_member(total, pair):
        field, pert = pair
        spec = jnp.dot(field.reshape(LEV * NLAT, NLON), forward, preferred_element_type=jnp.float32)
        spec = spec.astype(jnp.bfloat16).reshape(LEV, NLAT, 2, KEEP)
        coef = jnp.einsum('mnt,ltqm->lqmn', legendre_wide, spec.astype(jnp.float32))
        coef = (coef * response[None, None, :, :]).astype(jnp.bfloat16)
        synth = jnp.einsum('mnt,lqmn->ltqm', legendre_wide, coef.astype(jnp.float32)).astype(jnp.bfloat16)
        values = jnp.dot(synth.reshape(LEV * NLAT, 2 * KEEP), inverse, preferred_element_type=jnp.float32)
        values = values.reshape(LEV, NLAT, NLON)
        return (total + values * pert.astype(jnp.float32), None)
    start = jnp.zeros((LEV, NLAT, NLON), jnp.float32)
    total, unused = lax.scan(one_member, start, (alpha, perturbation))
    return total / jnp.sqrt(jnp.float32(members - 1))
```

```python
import functools
import math

import jax
import jax.numpy as jnp
import numpy as np
from jax import lax
from jax.experimental import pallas as pl
from jax.experimental.pallas import tpu as pltpu
from jax.sharding import PartitionSpec as P


def build_table(lon_count, keep_dev, grid_count):
    col = np.arange(2 * keep_dev * grid_count)
    block = col // (2 * keep_dev)
    part = col // keep_dev % 2
    wave = block * keep_dev + col % keep_dev
    phase = wave[:, None] * np.arange(lon_count)[None, :] % lon_count
    angle = phase.astype(np.float32) * np.float32(2.0 * math.pi / lon_count)
    basis = np.where(part[:, None] == 0, np.cos(angle), np.sin(angle))
    return jnp.asarray(basis.astype(jnp.bfloat16))


def legendre_filter(split, legendre, response):
    coef = jnp.einsum("mnt,qmkit->qmkin", legendre, split, preferred_element_type=jnp.float32)
    coef = (coef * response[None, :, None, None, :]).astype(jnp.bfloat16)
    synth = jnp.einsum("mnt,qmkin->qmkit", legendre, coef, preferred_element_type=jnp.float32)
    return synth.astype(jnp.bfloat16)


def reduce_levels(partial, levels):
    mem_count = lax.axis_size("mem")
    me = lax.axis_index("mem")
    owned = levels // mem_count
    if mem_count % 2:
        every = jnp.concatenate([partial(i * owned, owned) for i in range(mem_count)])
        return lax.psum_scatter(every, "mem", scatter_dimension=0, tiled=True)
    ring = mem_count // 2
    side, place = me % 2, me // 2
    swap = [(j, j ^ 1) for j in range(mem_count)]
    onward = [(j, (j + 2) % mem_count) for j in range(mem_count)]
    total = None
    for step in range(ring):
        goal = (place + 2 * ring - 1 - step) % ring
        give = partial((2 * goal + 1 - side) * owned, owned).astype(jnp.bfloat16)
        got = lax.ppermute(give, "mem", swap)
        here = partial((2 * goal + side) * owned, owned)
        here = here + got.astype(jnp.float32)
        if total is not None:
            here = here + total.astype(jnp.float32)
        if step < ring - 1:
            total = lax.ppermute(here.astype(jnp.bfloat16), "mem", onward)
    return here


def wave_rows(rows_ref, wave, waves, lat_dev):
    grid_count, parts, depth, _ = rows_ref.shape
    tiles = depth // waves
    per_pair = 2 * lat_dev // 128
    pairs = tiles // per_pair
    half = per_pair // 2
    lines = []
    for part in range(parts):
        even, odd = [], []
        for src in range(grid_count):
            block = rows_ref[src, part, pl.ds(wave, tiles, stride=waves), :]
            piece = [block[i * pairs : (i + 1) * pairs] for i in range(per_pair)]
            even += piece[:half] + [piece[half][:, :64]]
            odd += [piece[half][:, 64:]] + piece[half + 1 :]
        lines += [jnp.concatenate(even, axis=1), jnp.concatenate(odd, axis=1)]
    return jnp.concatenate(lines, axis=0)


def wave_back(back_ref, synth, wave, waves, lat_dev):
    grid_count, parts, depth, _ = back_ref.shape
    tiles = depth // waves
    per_pair = 2 * lat_dev // 128
    pairs = tiles // per_pair
    for part in range(parts):
        even = synth[2 * part * pairs : (2 * part + 1) * pairs]
        odd = synth[(2 * part + 1) * pairs : (2 * part + 2) * pairs]
        for src in range(grid_count):
            base = src * lat_dev
            both = jnp.concatenate(
                [even[:, base : base + lat_dev], odd[:, base : base + lat_dev]], axis=1
            )
            block = jnp.concatenate(
                [both[:, i * 128 : (i + 1) * 128] for i in range(per_pair)], axis=0
            )
            back_ref[src, part, pl.ds(wave, tiles, stride=waves), :] = block


def filter_waves(lat_dev, waves, first, x_ref, legendre_ref, response_ref, out_ref, rows_ref, back_ref):
    grid_count, parts, depth, _ = rows_ref.shape
    tiles = depth // waves
    per_pair = 2 * lat_dev // 128
    pairs = tiles // per_pair
    span = pl.ds(first, waves)
    group = 4
    height = 2 * parts * pairs

    def spot(tile):
        return (tile % per_pair) * pairs + tile // per_pair

    for src in range(grid_count):
        for part in range(parts):
            for tile in range(tiles):
                rows_ref[src, part, spot(tile) * waves : (spot(tile) + 1) * waves, :] = x_ref[
                    src, part, span, tile * 128 : (tile + 1) * 128
                ].astype(jnp.float32)

    def one_group(step, carry):
        wave = step * group
        field = jnp.concatenate(
            [wave_rows(rows_ref, wave + i, waves, lat_dev) for i in range(group)], axis=0
        ).astype(jnp.bfloat16)
        basis = legendre_ref[pl.ds(first + wave, group)]
        degrees, lat_count = basis.shape[1:]
        every = lax.dot_general(
            field, basis.reshape(group * degrees, lat_count), (((1,), (1,)), ((), ())),
            preferred_element_type=jnp.float32,
        )
        for i in range(group):
            coef = every[i * height : (i + 1) * height, i * degrees : (i + 1) * degrees]
            coef = (coef * response_ref[pl.ds(first + wave + i, 1), :]).astype(jnp.bfloat16)
            synth = jnp.dot(coef, legendre_ref[first + wave + i], preferred_element_type=jnp.float32)
            wave_back(back_ref, synth, wave + i, waves, lat_dev)
        return carry

    lax.fori_loop(0, waves // group, one_group, 0, unroll=2)
    for src in range(grid_count):
        for part in range(parts):
            for tile in range(tiles):
                out_ref[src, part, span, tile * 128 : (tile + 1) * 128] = back_ref[
                    src, part, spot(tile) * waves : (spot(tile) + 1) * waves, :
                ].astype(jnp.bfloat16)


def whole_kernel(
    order, waves, strips, alpha_ref, pert_ref, legendre_ref, response_ref, table_ref, out_ref,
    table_v, alpha_v, pert_v, basis_v, weight_v, spec_v, taken_v, made_v, result_v, rows_v, back_v,
    give_v, got_v, keep_v, pass_v, come_v,
    table_sem, basis_sem, alpha_sem, pert_sem, out_send, out_recv, back_send, back_recv,
    x_send, x_recv, z_send, z_recv,
):
    chunks, grid_count, parts, keep_dev, points = spec_v.shape
    mem_dev, _, lat_dev, lon_count = alpha_v.shape[1:]
    cols = grid_count * parts * keep_dev
    subs = keep_dev // waves
    deep = lat_dev // strips
    mem_count = 2 * chunks
    g = lax.axis_index("grid")
    me = lax.axis_index("mem")
    side, place = me % 2, me // 2
    top = chunks - 1
    peers = [lax.rem(g + d, grid_count) for d in range(1, grid_count)]
    across = me + 1 - 2 * side
    above = lax.rem(me + 2, mem_count)
    below = lax.rem(me + mem_count - 2, mem_count)

    def local(src, dst, sem):
        return pltpu.make_async_copy(src, dst, sem)

    def remote(src, dst, send, recv, where):
        return pltpu.make_async_remote_copy(
            src_ref=src, dst_ref=dst, send_sem=send, recv_sem=recv,
            device_id=where, device_id_type=pl.DeviceIdType.MESH,
        )

    def alpha_copy(c):
        return local(alpha_ref.at[:, pl.ds(2 * order[c], 2)], alpha_v.at[c], alpha_sem.at[c])

    def pert_copy(c):
        return local(pert_ref.at[:, pl.ds(2 * order[c], 2)], pert_v.at[c], pert_sem.at[c])

    def basis_copy(s):
        span = pl.ds(s * waves, waves)
        return local(legendre_ref.at[span], basis_v.at[span], basis_sem.at[s])

    def out_copy(c, d):
        return remote(
            spec_v.at[c, peers[d]], taken_v.at[c, g], out_send.at[c, d], out_recv.at[c, d], {"grid": peers[d]}
        )

    def back_copy(c, s, d):
        span = pl.ds(pl.multiple_of(s * waves, waves), waves)
        return remote(
            made_v.at[c, peers[d], :, span], result_v.at[c, g, :, span],
            back_send.at[c, s, d], back_recv.at[c, s, d], {"grid": peers[d]},
        )

    def rows(s):
        return pl.ds(s * deep, deep)

    def x_copy(c, s):
        return remote(
            give_v.at[c, rows(s)], got_v.at[c, rows(s)], x_send.at[c, s], x_recv.at[c, s], {"mem": across}
        )

    def z_copy(c, s, up):
        way = 0 if up else 1
        return remote(
            pass_v.at[c, rows(s)], come_v.at[c, way, rows(s)], z_send.at[c, way, s], z_recv.at[c, way, s],
            {"mem": above if up else below},
        )

    local(table_ref, table_v, table_sem.at[0]).start()
    alpha_copy(0).start()
    barrier = pltpu.get_barrier_semaphore()
    for peer in peers:
        pl.semaphore_signal(barrier, inc=1, device_id={"grid": peer}, device_id_type=pl.DeviceIdType.MESH)
    pl.semaphore_signal(barrier, inc=1, device_id={"mem": across}, device_id_type=pl.DeviceIdType.MESH)

    @pl.when(place < top)
    def _():
        pl.semaphore_signal(barrier, inc=1, device_id={"mem": above}, device_id_type=pl.DeviceIdType.MESH)

    @pl.when(place > 0)
    def _():
        pl.semaphore_signal(barrier, inc=1, device_id={"mem": below}, device_id_type=pl.DeviceIdType.MESH)

    alpha_copy(1).start()
    for s in range(subs):
        basis_copy(s).start()
    for c in range(2, chunks):
        alpha_copy(c).start()
    for c in range(chunks):
        pert_copy(c).start()

    wave = lax.broadcasted_iota(jnp.int32, weight_v.shape, 0) + g * keep_dev
    weight_v[...] = response_ref[...] * jnp.where(wave == 0, 1.0, 2.0).astype(jnp.float32)

    def spectra(c):
        if c == 0:
            local(table_ref, table_v, table_sem.at[0]).wait()
        alpha_copy(c).wait()
        spec = lax.dot_general(
            table_v[...], alpha_v[c].reshape(points, lon_count), (((1,), (1,)), ((), ())),
            preferred_element_type=jnp.float32,
        ).astype(jnp.bfloat16)
        spec_v[c] = spec.reshape(grid_count, parts, keep_dev, points)

    def send_out(c):
        for d in range(grid_count - 1):
            out_copy(c, d).start()

    def legendre(c):
        for d in range(grid_count - 1):
            out_copy(c, d).wait_recv()
        taken_v[c, g] = spec_v[c, g]
        if c == 0:
            for s in range(subs):
                basis_copy(s).wait()

        def one(s, carry):
            filter_waves(
                lat_dev, waves, pl.multiple_of(s * waves, waves), taken_v.at[c], basis_v, weight_v,
                made_v.at[c], rows_v, back_v,
            )
            for d in range(grid_count - 1):
                back_copy(c, s, d).start()
            return carry

        lax.fori_loop(0, subs, one, 0)
        result_v[c, g] = made_v[c, g]

    def synth(c):
        pert_copy(c).wait()
        for s in range(subs):
            for d in range(grid_count - 1):
                back_copy(c, s, d).wait_recv()
        field = result_v[c].reshape(cols, points)
        wide = 256 if lon_count % 256 == 0 else lon_count
        for left in range(0, lon_count, wide):
            cut = slice(left, left + wide)
            both = [None, None]
            for k in range(mem_dev):
                values = lax.dot_general(
                    field[:, 2 * k * lat_dev : 2 * (k + 1) * lat_dev], table_v[:, cut],
                    (((0,), (0,)), ((), ())), preferred_element_type=jnp.float32,
                )
                for i in range(2):
                    term = values[i * lat_dev : (i + 1) * lat_dev] * pert_v[c, k, i, :, cut].astype(jnp.float32)
                    both[i] = term if k == 0 else both[i] + term
            give_v[c, :, cut] = jnp.where(side == 0, both[1], both[0]).astype(jnp.bfloat16)
            keep_v[c, :, cut] = jnp.where(side == 0, both[0], both[1])
        for s in range(strips):
            x_copy(c, s).start()

    def pair_up(c, s):
        x_copy(c, s).wait_recv()
        keep_v[c, rows(s)] = keep_v[c, rows(s)] + got_v[c, rows(s)].astype(jnp.float32)
        p = order[c]
        if p > 0:
            @pl.when(place == 0)
            def _():
                pass_v[c, rows(s)] = keep_v[c, rows(s)].astype(jnp.bfloat16)
                z_copy(c, s, True).start()
        if p < top:
            @pl.when(place == top)
            def _():
                pass_v[c, rows(s)] = keep_v[c, rows(s)].astype(jnp.bfloat16)
                z_copy(c, s, False).start()

    def line(c, s):
        p = order[c]

        def forward(up):
            z_copy(c, s, up).wait_recv()
            way = 0 if up else 1
            pass_v[c, rows(s)] = (
                keep_v[c, rows(s)] + come_v[c, way, rows(s)].astype(jnp.float32)
            ).astype(jnp.bfloat16)
            z_copy(c, s, up).start()

        if p > 1:
            @pl.when((place > 0) & (place < p))
            def _():
                forward(True)
        if p < top - 1:
            @pl.when((place > p) & (place < top))
            def _():
                forward(False)

        @pl.when(place == p)
        def _():
            total = keep_v[c, rows(s)]
            if p > 0:
                z_copy(c, s, True).wait_recv()
                total = total + come_v[c, 0, rows(s)].astype(jnp.float32)
            if p < top:
                z_copy(c, s, False).wait_recv()
                total = total + come_v[c, 1, rows(s)].astype(jnp.float32)
            out_ref[0, rows(s)] = total

    spectra(0)
    need = grid_count + (place < top).astype(jnp.int32) + (place > 0).astype(jnp.int32)
    pl.semaphore_wait(barrier, need)
    send_out(0)
    spectra(1)
    send_out(1)
    for c in range(2, chunks):
        spectra(c)
    for c in range(chunks):
        legendre(c)
        if c + 2 < chunks:
            send_out(c + 2)
        if c > 0:
            synth(c - 1)
        if c > 1:
            for s in range(strips):
                pair_up(c - 2, s)
    for c in range(chunks - 1, chunks):
        synth(c)
    for c in range(max(chunks - 2, 0)):
        for s in range(strips):
            line(c, s)
    for c in range(max(chunks - 2, 0), chunks):
        for s in range(strips):
            pair_up(c, s)
            line(c, s)
    for c in range(chunks):
        p = order[c]
        for d in range(grid_count - 1):
            out_copy(c, d).wait_send()
            for s in range(subs):
                back_copy(c, s, d).wait_send()
        for s in range(strips):
            x_copy(c, s).wait_send()
        if p > 0:
            @pl.when(place < p)
            def _():
                for s in range(strips):
                    z_copy(c, s, True).wait_send()
        if p < top:
            @pl.when(place > p)
            def _():
                for s in range(strips):
                    z_copy(c, s, False).wait_send()


def whole(alpha, perturbation, legendre, response, table):
    mem_dev, levels, lat_dev, lon_count = alpha.shape
    keep_dev, degrees, lat_count = legendre.shape
    cols = table.shape[0]
    grid_count = cols // (2 * keep_dev)
    chunks = levels // 2
    points = mem_dev * 2 * lat_dev
    waves = 16
    subs = keep_dev // waves
    strips = 2
    order = []
    for i in range((chunks + 1) // 2):
        order += [i] if i == chunks - 1 - i else [i, chunks - 1 - i]
    half, wide = jnp.bfloat16, jnp.float32
    fields = pltpu.VMEM((chunks, mem_dev, 2, lat_dev, lon_count), half)
    waved = pltpu.VMEM((chunks, grid_count, 2, keep_dev, points), half)
    turned = pltpu.VMEM((grid_count, 2, points // 128 * waves, 128), wide)
    level = (chunks, lat_dev, lon_count)
    dma = pltpu.SemaphoreType.DMA
    peers = grid_count - 1
    return pl.pallas_call(
        functools.partial(whole_kernel, order, waves, strips),
        out_shape=jax.ShapeDtypeStruct((1, lat_dev, lon_count), wide),
        in_specs=[
            pl.BlockSpec(memory_space=pl.ANY),
            pl.BlockSpec(memory_space=pl.ANY),
            pl.BlockSpec(memory_space=pl.ANY),
            pl.BlockSpec(memory_space=pltpu.VMEM),
            pl.BlockSpec(memory_space=pl.ANY),
        ],
        out_specs=pl.BlockSpec(memory_space=pltpu.VMEM),
        scratch_shapes=[
            pltpu.VMEM((cols, lon_count), half), fields, fields,
            pltpu.VMEM((keep_dev, degrees, lat_count), half), pltpu.VMEM((keep_dev, degrees), wide),
            waved, waved, waved, waved, turned, turned,
            pltpu.VMEM(level, half), pltpu.VMEM(level, half), pltpu.VMEM(level, wide), pltpu.VMEM(level, half),
            pltpu.VMEM((chunks, 2, lat_dev, lon_count), half),
            dma((1,)), dma((subs,)), dma((chunks,)), dma((chunks,)),
            dma((chunks, peers)), dma((chunks, peers)), dma((chunks, subs, peers)), dma((chunks, subs, peers)),
            dma((chunks, strips)), dma((chunks, strips)), dma((chunks, 2, strips)), dma((chunks, 2, strips)),
        ],
        compiler_params=pltpu.CompilerParams(
            vmem_limit_bytes=63 * 2**20, collective_id=0, has_side_effects=True
        ),
        cost_estimate=pl.CostEstimate(
            flops=2**35, bytes_accessed=2 * alpha.size, transcendentals=0
        ),
    )(alpha, perturbation, legendre, response, table)


def body(alpha, perturbation, legendre, response):
    mem_dev, levels, lat_dev, lon_count = alpha.shape
    keep_dev = legendre.shape[0]
    grid_count = lax.axis_size("grid")
    members = mem_dev * lax.axis_size("mem")
    cols = 2 * keep_dev
    table = build_table(lon_count, keep_dev, grid_count)
    scale = jnp.float32(1.0 / (lon_count * math.sqrt(members - 1)))
    if keep_dev % 16 == 0 and lat_dev % 128 == 64 and levels == lax.axis_size("mem") and levels in (4, 6, 8):
        return whole(alpha, perturbation, legendre, response, table) * scale

    wave = lax.axis_index("grid") * keep_dev + jnp.arange(keep_dev)
    response = response * jnp.where(wave == 0, 1.0, 2.0).astype(jnp.float32)[:, None]

    points = mem_dev * levels * lat_dev
    lane = math.gcd(points, 128)
    spectra = jnp.einsum("cx,klyx->ckly", table, alpha, preferred_element_type=jnp.float32)
    spectra = spectra.astype(jnp.bfloat16).reshape(grid_count, cols, points // lane, lane)
    spectra = lax.all_to_all(spectra, "grid", split_axis=0, concat_axis=0, tiled=True)
    split = spectra.reshape(grid_count, 2, keep_dev, mem_dev, levels, lat_dev)
    split = jnp.transpose(split, (1, 2, 3, 4, 0, 5)).reshape(2, keep_dev, mem_dev, levels, -1)
    filtered = legendre_filter(split, legendre, response)
    filtered = filtered.reshape(2, keep_dev, mem_dev, levels, grid_count, lat_dev)
    filtered = jnp.transpose(filtered, (4, 0, 1, 2, 3, 5)).reshape(grid_count, cols, points // lane, lane)
    filtered = lax.all_to_all(filtered, "grid", split_axis=0, concat_axis=0, tiled=True)
    filtered = filtered.reshape(grid_count * cols, mem_dev, levels, lat_dev)
    filtered = jnp.transpose(filtered, (1, 2, 3, 0))

    def partial(level, count):
        field = lax.dynamic_slice_in_dim(filtered, level, count, 1)
        weight = lax.dynamic_slice_in_dim(perturbation, level, count, 1)
        values = jnp.einsum("klyc,cx->klyx", field, table, preferred_element_type=jnp.float32)
        return jnp.sum(values * weight, axis=0)

    total = reduce_levels(partial, levels)
    return total * scale


def solution(mesh):
    placed = (
        P("mem", None, "grid", None),
        P("mem", None, "grid", None),
        P("grid", None, None),
        P("grid", None),
    )
    return jax.shard_map(
        body, mesh=mesh, in_specs=placed, out_specs=P("mem", "grid", None), check_vma=False
    )
```

```python
import functools
import math

import jax
import jax.numpy as jnp
import numpy as np
from jax import lax
from jax.experimental import pallas as pl
from jax.experimental.pallas import tpu as pltpu
from jax.sharding import PartitionSpec as P


def build_table(lon_count, keep_dev, grid_count):
    col = np.arange(2 * keep_dev * grid_count)
    block = col // (2 * keep_dev)
    part = col // keep_dev % 2
    wave = block * keep_dev + col % keep_dev
    phase = wave[:, None] * np.arange(lon_count)[None, :] % lon_count
    angle = phase.astype(np.float32) * np.float32(2.0 * math.pi / lon_count)
    basis = np.where(part[:, None] == 0, np.cos(angle), np.sin(angle))
    return jnp.asarray(basis.astype(jnp.bfloat16))


def legendre_filter(split, legendre, response):
    coef = jnp.einsum("mnt,qmkit->qmkin", legendre, split, preferred_element_type=jnp.float32)
    coef = (coef * response[None, :, None, None, :]).astype(jnp.bfloat16)
    synth = jnp.einsum("mnt,qmkin->qmkit", legendre, coef, preferred_element_type=jnp.float32)
    return synth.astype(jnp.bfloat16)


def reduce_levels(partial, levels):
    mem_count = lax.axis_size("mem")
    me = lax.axis_index("mem")
    owned = levels // mem_count
    if mem_count % 2:
        every = jnp.concatenate([partial(i * owned, owned) for i in range(mem_count)])
        return lax.psum_scatter(every, "mem", scatter_dimension=0, tiled=True)
    ring = mem_count // 2
    side, place = me % 2, me // 2
    swap = [(j, j ^ 1) for j in range(mem_count)]
    onward = [(j, (j + 2) % mem_count) for j in range(mem_count)]
    total = None
    for step in range(ring):
        goal = (place + 2 * ring - 1 - step) % ring
        give = partial((2 * goal + 1 - side) * owned, owned).astype(jnp.bfloat16)
        got = lax.ppermute(give, "mem", swap)
        here = partial((2 * goal + side) * owned, owned)
        here = here + got.astype(jnp.float32)
        if total is not None:
            here = here + total.astype(jnp.float32)
        if step < ring - 1:
            total = lax.ppermute(here.astype(jnp.bfloat16), "mem", onward)
    return here


def wave_rows(rows_ref, wave, waves, lat_dev):
    grid_count, parts, depth, _ = rows_ref.shape
    tiles = depth // waves
    per_pair = 2 * lat_dev // 128
    pairs = tiles // per_pair
    half = per_pair // 2
    lines = []
    for part in range(parts):
        even, odd = [], []
        for src in range(grid_count):
            block = rows_ref[src, part, pl.ds(wave, tiles, stride=waves), :]
            piece = [block[i * pairs : (i + 1) * pairs] for i in range(per_pair)]
            even += piece[:half] + [piece[half][:, :64]]
            odd += [piece[half][:, 64:]] + piece[half + 1 :]
        lines += [jnp.concatenate(even, axis=1), jnp.concatenate(odd, axis=1)]
    return jnp.concatenate(lines, axis=0)


def wave_back(back_ref, synth, wave, waves, lat_dev):
    grid_count, parts, depth, _ = back_ref.shape
    tiles = depth // waves
    per_pair = 2 * lat_dev // 128
    pairs = tiles // per_pair
    for part in range(parts):
        even = synth[2 * part * pairs : (2 * part + 1) * pairs]
        odd = synth[(2 * part + 1) * pairs : (2 * part + 2) * pairs]
        for src in range(grid_count):
            base = src * lat_dev
            both = jnp.concatenate(
                [even[:, base : base + lat_dev], odd[:, base : base + lat_dev]], axis=1
            )
            block = jnp.concatenate(
                [both[:, i * 128 : (i + 1) * 128] for i in range(per_pair)], axis=0
            )
            back_ref[src, part, pl.ds(wave, tiles, stride=waves), :] = block


def filter_waves(lat_dev, waves, first, x_ref, legendre_ref, response_ref, out_ref, rows_ref, back_ref):
    grid_count, parts, depth, _ = rows_ref.shape
    tiles = depth // waves
    per_pair = 2 * lat_dev // 128
    pairs = tiles // per_pair
    span = pl.ds(first, waves)
    group = 4
    height = 2 * parts * pairs

    def spot(tile):
        return (tile % per_pair) * pairs + tile // per_pair

    for src in range(grid_count):
        for part in range(parts):
            for tile in range(tiles):
                rows_ref[src, part, spot(tile) * waves : (spot(tile) + 1) * waves, :] = x_ref[
                    src, part, span, tile * 128 : (tile + 1) * 128
                ].astype(jnp.float32)

    def one_group(step, carry):
        wave = step * group
        field = jnp.concatenate(
            [wave_rows(rows_ref, wave + i, waves, lat_dev) for i in range(group)], axis=0
        ).astype(jnp.bfloat16)
        basis = legendre_ref[pl.ds(first + wave, group)]
        degrees, lat_count = basis.shape[1:]
        every = lax.dot_general(
            field, basis.reshape(group * degrees, lat_count), (((1,), (1,)), ((), ())),
            preferred_element_type=jnp.float32,
        )
        for i in range(group):
            coef = every[i * height : (i + 1) * height, i * degrees : (i + 1) * degrees]
            coef = (coef * response_ref[pl.ds(first + wave + i, 1), :]).astype(jnp.bfloat16)
            synth = jnp.dot(coef, legendre_ref[first + wave + i], preferred_element_type=jnp.float32)
            wave_back(back_ref, synth, wave + i, waves, lat_dev)
        return carry

    lax.fori_loop(0, waves // group, one_group, 0, unroll=2)
    for src in range(grid_count):
        for part in range(parts):
            for tile in range(tiles):
                out_ref[src, part, span, tile * 128 : (tile + 1) * 128] = back_ref[
                    src, part, spot(tile) * waves : (spot(tile) + 1) * waves, :
                ].astype(jnp.bfloat16)


def whole_kernel(
    order, waves, strips, alpha_ref, pert_ref, legendre_ref, response_ref, table_ref, out_ref,
    table_v, alpha_v, pert_v, basis_v, weight_v, spec_v, taken_v, made_v, result_v, rows_v, back_v,
    give_v, got_v, keep_v, pass_v, come_v,
    table_sem, basis_sem, alpha_sem, pert_sem, out_send, out_recv, back_send, back_recv,
    x_send, x_recv, z_send, z_recv,
):
    chunks, grid_count, parts, keep_dev, points = spec_v.shape
    mem_dev, _, lat_dev, lon_count = alpha_v.shape[1:]
    cols = grid_count * parts * keep_dev
    subs = keep_dev // waves
    deep = lat_dev // strips
    mem_count = 2 * chunks
    g = lax.axis_index("grid")
    me = lax.axis_index("mem")
    side, place = me % 2, me // 2
    top = chunks - 1
    peers = [lax.rem(g + d, grid_count) for d in range(1, grid_count)]
    across = me + 1 - 2 * side
    above = lax.rem(me + 2, mem_count)
    below = lax.rem(me + mem_count - 2, mem_count)

    def local(src, dst, sem):
        return pltpu.make_async_copy(src, dst, sem)

    def remote(src, dst, send, recv, where):
        return pltpu.make_async_remote_copy(
            src_ref=src, dst_ref=dst, send_sem=send, recv_sem=recv,
            device_id=where, device_id_type=pl.DeviceIdType.MESH,
        )

    def alpha_copy(c):
        return local(alpha_ref.at[:, pl.ds(2 * order[c], 2)], alpha_v.at[c % 2], alpha_sem.at[c])

    def pert_copy(c):
        return local(pert_ref.at[:, pl.ds(2 * order[c], 2)], pert_v.at[c], pert_sem.at[c])

    def basis_copy(s):
        span = pl.ds(s * waves, waves)
        return local(legendre_ref.at[span], basis_v.at[span], basis_sem.at[s])

    def out_copy(c, s, d):
        span = pl.ds(s * waves, waves)
        return remote(
            spec_v.at[c, peers[d], :, span], taken_v.at[c, g, :, span],
            out_send.at[c, s, d], out_recv.at[c, s, d], {"grid": peers[d]},
        )

    def back_copy(c, s, d):
        span = pl.ds(s * waves, waves)
        return remote(
            made_v.at[c, peers[d], :, span], result_v.at[c, g, :, span],
            back_send.at[c, s, d], back_recv.at[c, s, d], {"grid": peers[d]},
        )

    def rows(s):
        return pl.ds(s * deep, deep)

    def x_copy(c, s):
        return remote(
            give_v.at[c, rows(s)], got_v.at[c, rows(s)], x_send.at[c, s], x_recv.at[c, s], {"mem": across}
        )

    def z_copy(c, s, up):
        way = 0 if up else 1
        return remote(
            pass_v.at[c, rows(s)], come_v.at[c, way, rows(s)], z_send.at[c, way, s], z_recv.at[c, way, s],
            {"mem": above if up else below},
        )

    local(table_ref, table_v, table_sem.at[0]).start()
    alpha_copy(0).start()
    barrier = pltpu.get_barrier_semaphore()
    for peer in peers:
        pl.semaphore_signal(barrier, inc=1, device_id={"grid": peer}, device_id_type=pl.DeviceIdType.MESH)
    pl.semaphore_signal(barrier, inc=1, device_id={"mem": across}, device_id_type=pl.DeviceIdType.MESH)

    @pl.when(place < top)
    def _():
        pl.semaphore_signal(barrier, inc=1, device_id={"mem": above}, device_id_type=pl.DeviceIdType.MESH)

    @pl.when(place > 0)
    def _():
        pl.semaphore_signal(barrier, inc=1, device_id={"mem": below}, device_id_type=pl.DeviceIdType.MESH)

    local(response_ref, weight_v, table_sem.at[1]).start()
    alpha_copy(1).start()

    def spectra(c):
        if c == 0:
            local(table_ref, table_v, table_sem.at[0]).wait()
        alpha_copy(c).wait()
        if c == 0:
            for s in range(subs):
                basis_copy(s).start()
        spec = lax.dot_general(
            table_v[...], alpha_v[c % 2].reshape(points, lon_count), (((1,), (1,)), ((), ())),
            preferred_element_type=jnp.float32,
        ).astype(jnp.bfloat16)
        spec_v[c] = spec.reshape(grid_count, parts, keep_dev, points)
        taken_v[c, g] = spec_v[c, g]
        if c + 2 < chunks:
            alpha_copy(c + 2).start()

    def send_out(c):
        for s in range(subs):
            for d in range(grid_count - 1):
                out_copy(c, s, d).start()

    def legendre(c, s):
        if c == 0:
            basis_copy(s).wait()
            pert_copy(s).start()
            if s == subs - 1:
                for other in range(subs, chunks):
                    pert_copy(other).start()
        for d in range(grid_count - 1):
            out_copy(c, s, d).wait_recv()
        filter_waves(
            lat_dev, waves, s * waves, taken_v.at[c], basis_v, weight_v, made_v.at[c], rows_v, back_v
        )
        for d in range(grid_count - 1):
            back_copy(c, s, d).start()
        if s == subs - 1:
            if c + 1 < chunks:
                send_out(c + 1)
            result_v[c, g] = made_v[c, g]

    def synth(c):
        pert_copy(c).wait()
        for s in range(subs):
            for d in range(grid_count - 1):
                back_copy(c, s, d).wait_recv()
        field = result_v[c].reshape(cols, points)
        wide = 256 if lon_count % 256 == 0 else lon_count
        for left in range(0, lon_count, wide):
            cut = slice(left, left + wide)
            both = [None, None]
            for k in range(mem_dev):
                values = lax.dot_general(
                    field[:, 2 * k * lat_dev : 2 * (k + 1) * lat_dev], table_v[:, cut],
                    (((0,), (0,)), ((), ())), preferred_element_type=jnp.float32,
                )
                for i in range(2):
                    term = values[i * lat_dev : (i + 1) * lat_dev] * pert_v[c, k, i, :, cut].astype(jnp.float32)
                    both[i] = term if k == 0 else both[i] + term
            give_v[c, :, cut] = jnp.where(side == 0, both[1], both[0]).astype(jnp.bfloat16)
            keep_v[c, :, cut] = jnp.where(side == 0, both[0], both[1])
        for s in range(strips):
            x_copy(c, s).start()

    def gather(c, s, z):
        p = order[c]
        x_copy(c, s).wait_recv()
        total = keep_v[c, rows(s)] + got_v[c, rows(s)].astype(jnp.float32)
        for way in range(2):
            up = way == 0
            if (0 < z <= p) if up else (p <= z < top):
                z_copy(c, s, up).wait_recv()
                total = total + come_v[c, way, rows(s)].astype(jnp.float32)
        if z == p:
            out_ref[0, rows(s)] = total
        else:
            pass_v[c, rows(s)] = total.astype(jnp.bfloat16)
            z_copy(c, s, z < p).start()

    steps = []
    for c in range(chunks):
        p = order[c]
        begin = 12.8 * c
        steps += [(8.4 + begin + 2.2 * s, legendre, (c, s)) for s in range(subs)]
        steps.append((19.1 + begin, synth, (c,)))
        if c > 0:
            steps.append((3.0 + 6.3 * c, spectra, (c,)))
        for z in range(chunks):
            hops = z if z < p else top - z if z > p else max(p, top - p)
            slack = 0.0 if c == chunks - 1 else 1.5
            for s in range(strips):
                ready = 23.0 + slack + begin + 12.7 * (s + 1) / strips + hops * (2.8 + slack + 12.7 / strips)
                steps.append((ready, gather, (c, s, z)))
    steps.sort(key=lambda step: step[0])

    spectra(0)
    local(response_ref, weight_v, table_sem.at[1]).wait()
    wave = lax.broadcasted_iota(jnp.int32, weight_v.shape, 0) + g * keep_dev
    weight_v[...] = weight_v[...] * jnp.where(wave == 0, 1.0, 2.0).astype(jnp.float32)
    need = grid_count + (place < top).astype(jnp.int32) + (place > 0).astype(jnp.int32)
    pl.semaphore_wait(barrier, need)
    send_out(0)
    steps = [step for step in steps if step[1] is spectra and step[2] == (1,)] + [
        step for step in steps if not (step[1] is spectra and step[2] == (1,))
    ]
    for _, act, which in steps:
        if act is gather:
            pl.when(place == which[2])(functools.partial(gather, *which))
        else:
            act(*which)
    for c in range(chunks):
        p = order[c]
        for d in range(grid_count - 1):
            for s in range(subs):
                out_copy(c, s, d).wait_send()
                back_copy(c, s, d).wait_send()
        for s in range(strips):
            x_copy(c, s).wait_send()
        if p > 0:
            @pl.when(place < p)
            def _():
                for s in range(strips):
                    z_copy(c, s, True).wait_send()
        if p < top:
            @pl.when(place > p)
            def _():
                for s in range(strips):
                    z_copy(c, s, False).wait_send()


def whole(alpha, perturbation, legendre, response, table):
    mem_dev, levels, lat_dev, lon_count = alpha.shape
    keep_dev, degrees, lat_count = legendre.shape
    cols = table.shape[0]
    grid_count = cols // (2 * keep_dev)
    chunks = levels // 2
    points = mem_dev * 2 * lat_dev
    waves = 16
    subs = keep_dev // waves
    strips = 4
    order = list(range(1, chunks, 2)) + list(range(0, chunks, 2))
    half, wide = jnp.bfloat16, jnp.float32
    field = (mem_dev, 2, lat_dev, lon_count)
    waved = pltpu.VMEM((chunks, grid_count, 2, keep_dev, points), half)
    turned = pltpu.VMEM((grid_count, 2, points // 128 * waves, 128), wide)
    level = (chunks, lat_dev, lon_count)
    dma = pltpu.SemaphoreType.DMA
    peers = grid_count - 1
    return pl.pallas_call(
        functools.partial(whole_kernel, order, waves, strips),
        out_shape=jax.ShapeDtypeStruct((1, lat_dev, lon_count), wide),
        in_specs=[
            pl.BlockSpec(memory_space=pl.ANY),
            pl.BlockSpec(memory_space=pl.ANY),
            pl.BlockSpec(memory_space=pl.ANY),
            pl.BlockSpec(memory_space=pl.ANY),
            pl.BlockSpec(memory_space=pl.ANY),
        ],
        out_specs=pl.BlockSpec(memory_space=pltpu.VMEM),
        scratch_shapes=[
            pltpu.VMEM((cols, lon_count), half), pltpu.VMEM((2,) + field, half), pltpu.VMEM((chunks,) + field, half),
            pltpu.VMEM((keep_dev, degrees, lat_count), half), pltpu.VMEM((keep_dev, degrees), wide),
            waved, waved, waved, waved, turned, turned,
            pltpu.VMEM(level, half), pltpu.VMEM(level, half), pltpu.VMEM(level, wide), pltpu.VMEM(level, half),
            pltpu.VMEM((chunks, 2, lat_dev, lon_count), half),
            dma((2,)), dma((subs,)), dma((chunks,)), dma((chunks,)),
            dma((chunks, subs, peers)), dma((chunks, subs, peers)), dma((chunks, subs, peers)), dma((chunks, subs, peers)),
            dma((chunks, strips)), dma((chunks, strips)), dma((chunks, 2, strips)), dma((chunks, 2, strips)),
        ],
        compiler_params=pltpu.CompilerParams(
            vmem_limit_bytes=53 * 2**20, collective_id=0, has_side_effects=True
        ),
        cost_estimate=pl.CostEstimate(
            flops=2**35, bytes_accessed=2 * alpha.size, transcendentals=0
        ),
    )(alpha, perturbation, legendre, response, table)


def body(alpha, perturbation, legendre, response):
    mem_dev, levels, lat_dev, lon_count = alpha.shape
    keep_dev = legendre.shape[0]
    grid_count = lax.axis_size("grid")
    members = mem_dev * lax.axis_size("mem")
    cols = 2 * keep_dev
    table = build_table(lon_count, keep_dev, grid_count)
    scale = jnp.float32(1.0 / (lon_count * math.sqrt(members - 1)))
    if keep_dev % 16 == 0 and lat_dev % 128 == 64 and levels == lax.axis_size("mem") and levels in (4, 6, 8):
        return whole(alpha, perturbation, legendre, response, table) * scale

    wave = lax.axis_index("grid") * keep_dev + jnp.arange(keep_dev)
    response = response * jnp.where(wave == 0, 1.0, 2.0).astype(jnp.float32)[:, None]

    points = mem_dev * levels * lat_dev
    lane = math.gcd(points, 128)
    spectra = jnp.einsum("cx,klyx->ckly", table, alpha, preferred_element_type=jnp.float32)
    spectra = spectra.astype(jnp.bfloat16).reshape(grid_count, cols, points // lane, lane)
    spectra = lax.all_to_all(spectra, "grid", split_axis=0, concat_axis=0, tiled=True)
    split = spectra.reshape(grid_count, 2, keep_dev, mem_dev, levels, lat_dev)
    split = jnp.transpose(split, (1, 2, 3, 4, 0, 5)).reshape(2, keep_dev, mem_dev, levels, -1)
    filtered = legendre_filter(split, legendre, response)
    filtered = filtered.reshape(2, keep_dev, mem_dev, levels, grid_count, lat_dev)
    filtered = jnp.transpose(filtered, (4, 0, 1, 2, 3, 5)).reshape(grid_count, cols, points // lane, lane)
    filtered = lax.all_to_all(filtered, "grid", split_axis=0, concat_axis=0, tiled=True)
    filtered = filtered.reshape(grid_count * cols, mem_dev, levels, lat_dev)
    filtered = jnp.transpose(filtered, (1, 2, 3, 0))

    def partial(level, count):
        field = lax.dynamic_slice_in_dim(filtered, level, count, 1)
        weight = lax.dynamic_slice_in_dim(perturbation, level, count, 1)
        values = jnp.einsum("klyc,cx->klyx", field, table, preferred_element_type=jnp.float32)
        return jnp.sum(values * weight, axis=0)

    total = reduce_levels(partial, levels)
    return total * scale


def solution(mesh):
    placed = (
        P("mem", None, "grid", None),
        P("mem", None, "grid", None),
        P("grid", None, None),
        P("grid", None),
    )
    return jax.shard_map(
        body, mesh=mesh, in_specs=placed, out_specs=P("mem", "grid", None), check_vma=False
    )
```

```python
import functools
import math

import jax
import jax.numpy as jnp
import numpy as np
from jax import lax
from jax.experimental import pallas as pl
from jax.experimental.pallas import tpu as pltpu
from jax.sharding import PartitionSpec as P


def build_table(lon_count, keep_dev, grid_count):
    col = np.arange(2 * keep_dev * grid_count)
    block = col // (2 * keep_dev)
    part = col // keep_dev % 2
    wave = block * keep_dev + col % keep_dev
    phase = wave[:, None] * np.arange(lon_count)[None, :] % lon_count
    angle = phase.astype(np.float32) * np.float32(2.0 * math.pi / lon_count)
    basis = np.where(part[:, None] == 0, np.cos(angle), np.sin(angle))
    return jnp.asarray(basis.astype(jnp.bfloat16))


def legendre_filter(split, legendre, response):
    coef = jnp.einsum("mnt,qmkit->qmkin", legendre, split, preferred_element_type=jnp.float32)
    coef = (coef * response[None, :, None, None, :]).astype(jnp.bfloat16)
    synth = jnp.einsum("mnt,qmkin->qmkit", legendre, coef, preferred_element_type=jnp.float32)
    return synth.astype(jnp.bfloat16)


def reduce_levels(partial, levels):
    mem_count = lax.axis_size("mem")
    me = lax.axis_index("mem")
    owned = levels // mem_count
    if mem_count % 2:
        every = jnp.concatenate([partial(i * owned, owned) for i in range(mem_count)])
        return lax.psum_scatter(every, "mem", scatter_dimension=0, tiled=True)
    ring = mem_count // 2
    side, place = me % 2, me // 2
    swap = [(j, j ^ 1) for j in range(mem_count)]
    onward = [(j, (j + 2) % mem_count) for j in range(mem_count)]
    total = None
    for step in range(ring):
        goal = (place + 2 * ring - 1 - step) % ring
        give = partial((2 * goal + 1 - side) * owned, owned).astype(jnp.bfloat16)
        got = lax.ppermute(give, "mem", swap)
        here = partial((2 * goal + side) * owned, owned)
        here = here + got.astype(jnp.float32)
        if total is not None:
            here = here + total.astype(jnp.float32)
        if step < ring - 1:
            total = lax.ppermute(here.astype(jnp.bfloat16), "mem", onward)
    return here


def wave_rows(rows_ref, wave, waves, lat_dev):
    grid_count, parts, depth, _ = rows_ref.shape
    tiles = depth // waves
    per_pair = 2 * lat_dev // 128
    pairs = tiles // per_pair
    half = per_pair // 2
    lines = []
    for part in range(parts):
        even, odd = [], []
        for src in range(grid_count):
            block = rows_ref[src, part, pl.ds(wave, tiles, stride=waves), :]
            piece = [block[i * pairs : (i + 1) * pairs] for i in range(per_pair)]
            even += piece[:half] + [piece[half][:, :64]]
            odd += [piece[half][:, 64:]] + piece[half + 1 :]
        lines += [jnp.concatenate(even, axis=1), jnp.concatenate(odd, axis=1)]
    return jnp.concatenate(lines, axis=0)


def wave_back(back_ref, synth, wave, waves, lat_dev):
    grid_count, parts, depth, _ = back_ref.shape
    tiles = depth // waves
    per_pair = 2 * lat_dev // 128
    pairs = tiles // per_pair
    for part in range(parts):
        even = synth[2 * part * pairs : (2 * part + 1) * pairs]
        odd = synth[(2 * part + 1) * pairs : (2 * part + 2) * pairs]
        for src in range(grid_count):
            base = src * lat_dev
            both = jnp.concatenate(
                [even[:, base : base + lat_dev], odd[:, base : base + lat_dev]], axis=1
            )
            block = jnp.concatenate(
                [both[:, i * 128 : (i + 1) * 128] for i in range(per_pair)], axis=0
            )
            back_ref[src, part, pl.ds(wave, tiles, stride=waves), :] = block


def filter_waves(lat_dev, waves, first, x_ref, legendre_ref, response_ref, out_ref, rows_ref, back_ref):
    grid_count, parts, depth, _ = rows_ref.shape
    tiles = depth // waves
    per_pair = 2 * lat_dev // 128
    pairs = tiles // per_pair
    span = pl.ds(first, waves)
    group = 4
    height = 2 * parts * pairs

    def spot(tile):
        return (tile % per_pair) * pairs + tile // per_pair

    for src in range(grid_count):
        for part in range(parts):
            for tile in range(tiles):
                rows_ref[src, part, spot(tile) * waves : (spot(tile) + 1) * waves, :] = x_ref[
                    src, part, span, tile * 128 : (tile + 1) * 128
                ].astype(jnp.float32)

    def one_group(step, carry):
        wave = step * group
        field = jnp.concatenate(
            [wave_rows(rows_ref, wave + i, waves, lat_dev) for i in range(group)], axis=0
        ).astype(jnp.bfloat16)
        basis = legendre_ref[pl.ds(first + wave, group)]
        degrees, lat_count = basis.shape[1:]
        every = lax.dot_general(
            field, basis.reshape(group * degrees, lat_count), (((1,), (1,)), ((), ())),
            preferred_element_type=jnp.float32,
        )
        for i in range(group):
            coef = every[i * height : (i + 1) * height, i * degrees : (i + 1) * degrees]
            coef = (coef * response_ref[pl.ds(first + wave + i, 1), :]).astype(jnp.bfloat16)
            synth = jnp.dot(coef, legendre_ref[first + wave + i], preferred_element_type=jnp.float32)
            wave_back(back_ref, synth, wave + i, waves, lat_dev)
        return carry

    lax.fori_loop(0, waves // group, one_group, 0, unroll=2)
    for src in range(grid_count):
        for part in range(parts):
            for tile in range(tiles):
                out_ref[src, part, span, tile * 128 : (tile + 1) * 128] = back_ref[
                    src, part, spot(tile) * waves : (spot(tile) + 1) * waves, :
                ].astype(jnp.bfloat16)


def whole_kernel(
    order, waves, strips, alpha_ref, pert_ref, legendre_ref, response_ref, table_ref, out_ref,
    table_v, alpha_v, pert_v, basis_v, weight_v, spec_v, taken_v, made_v, result_v, rows_v, back_v,
    give_v, got_v, keep_v, pass_v, come_v, done_v,
    table_sem, first_sem, basis_sem, alpha_sem, pert_sem, out_send, out_recv, back_send, back_recv,
    x_send, x_recv, z_send, z_recv, done_sem,
):
    chunks, grid_count, parts, keep_dev, points = spec_v.shape
    mem_dev, _, lat_dev, lon_count = alpha_v.shape[1:]
    cols = grid_count * parts * keep_dev
    subs = keep_dev // waves
    mem_count = 2 * chunks
    g = lax.axis_index("grid")
    me = lax.axis_index("mem")
    side, place = me % 2, me // 2
    top = chunks - 1
    peers = [lax.rem(g + d, grid_count) for d in range(1, grid_count)]
    across = me + 1 - 2 * side
    above = lax.rem(me + 2, mem_count)
    below = lax.rem(me + mem_count - 2, mem_count)

    def local(src, dst, sem):
        return pltpu.make_async_copy(src, dst, sem)

    def remote(src, dst, send, recv, where):
        return pltpu.make_async_remote_copy(
            src_ref=src, dst_ref=dst, send_sem=send, recv_sem=recv,
            device_id=where, device_id_type=pl.DeviceIdType.MESH,
        )

    def alpha_copy(c):
        return local(alpha_ref.at[:, pl.ds(2 * order[c], 2)], alpha_v.at[c % 2], alpha_sem.at[c])

    def first_copy(k):
        return local(alpha_ref.at[k, pl.ds(2 * order[0], 2)], alpha_v.at[0, k], first_sem.at[k])

    def pert_copy(c):
        return local(pert_ref.at[:, pl.ds(2 * order[c], 2)], pert_v.at[c], pert_sem.at[c])

    def basis_copy(s):
        span = pl.ds(s * waves, waves)
        return local(legendre_ref.at[span], basis_v.at[span], basis_sem.at[s])

    def out_copy(c, s, d):
        span = pl.ds(s * waves, waves)
        return remote(
            spec_v.at[c, peers[d], :, span], taken_v.at[c, g, :, span],
            out_send.at[c, s, d], out_recv.at[c, s, d], {"grid": peers[d]},
        )

    def back_copy(c, s, d):
        span = pl.ds(s * waves, waves)
        return remote(
            made_v.at[c, peers[d], :, span], result_v.at[c, g, :, span],
            back_send.at[c, s, d], back_recv.at[c, s, d], {"grid": peers[d]},
        )

    def rows(c, s):
        deep = lat_dev // strips[c]
        return pl.ds(s * deep, deep)

    def x_copy(c, s):
        return remote(
            give_v.at[c, rows(c, s)], got_v.at[c, rows(c, s)], x_send.at[c, s], x_recv.at[c, s], {"mem": across}
        )

    def z_copy(c, s, up):
        way = 0 if up else 1
        return remote(
            pass_v.at[c, rows(c, s)], come_v.at[c, way, rows(c, s)], z_send.at[c, way, s], z_recv.at[c, way, s],
            {"mem": above if up else below},
        )

    def done_copy(c, s):
        return local(done_v.at[rows(c, s)], out_ref.at[0, rows(c, s)], done_sem.at[s])

    local(table_ref, table_v, table_sem.at[0]).start()
    for k in range(mem_dev):
        first_copy(k).start()
    barrier = pltpu.get_barrier_semaphore()
    for peer in peers:
        pl.semaphore_signal(barrier, inc=1, device_id={"grid": peer}, device_id_type=pl.DeviceIdType.MESH)
    pl.semaphore_signal(barrier, inc=1, device_id={"mem": across}, device_id_type=pl.DeviceIdType.MESH)

    @pl.when(place < top)
    def _():
        pl.semaphore_signal(barrier, inc=1, device_id={"mem": above}, device_id_type=pl.DeviceIdType.MESH)

    @pl.when(place > 0)
    def _():
        pl.semaphore_signal(barrier, inc=1, device_id={"mem": below}, device_id_type=pl.DeviceIdType.MESH)

    local(response_ref, weight_v, table_sem.at[1]).start()

    def spectra(c):
        if c == 0:
            local(table_ref, table_v, table_sem.at[0]).wait()
            lanes = points // mem_dev
            for k in range(mem_dev):
                first_copy(k).wait()
                if k == mem_dev - 1:
                    alpha_copy(1).start()
                spec = lax.dot_general(
                    table_v[...], alpha_v[0, k].reshape(lanes, lon_count), (((1,), (1,)), ((), ())),
                    preferred_element_type=jnp.float32,
                ).astype(jnp.bfloat16)
                spec_v[0, :, :, :, k * lanes : (k + 1) * lanes] = spec.reshape(
                    grid_count, parts, keep_dev, lanes
                )
            for s in range(subs):
                basis_copy(s).start()
        else:
            alpha_copy(c).wait()
            spec = lax.dot_general(
                table_v[...], alpha_v[c % 2].reshape(points, lon_count), (((1,), (1,)), ((), ())),
                preferred_element_type=jnp.float32,
            ).astype(jnp.bfloat16)
            spec_v[c] = spec.reshape(grid_count, parts, keep_dev, points)
        taken_v[c, g] = spec_v[c, g]
        if c + 2 < chunks:
            alpha_copy(c + 2).start()

    def send_out(c):
        for s in range(subs):
            for d in range(grid_count - 1):
                out_copy(c, s, d).start()

    def legendre(c, s):
        if c == 0:
            basis_copy(s).wait()
            pert_copy(s).start()
            if s == subs - 1:
                for other in range(subs, chunks):
                    pert_copy(other).start()
        for d in range(grid_count - 1):
            out_copy(c, s, d).wait_recv()
        filter_waves(
            lat_dev, waves, s * waves, taken_v.at[c], basis_v, weight_v, made_v.at[c], rows_v, back_v
        )
        for d in range(grid_count - 1):
            back_copy(c, s, d).start()
        if s == subs - 1:
            if c + 1 < chunks:
                send_out(c + 1)
            result_v[c, g] = made_v[c, g]

    def settle_grid(c):
        for s in range(subs):
            for d in range(grid_count - 1):
                out_copy(c, s, d).wait_send()
                back_copy(c, s, d).wait_send()

    def settle_pair(c):
        for s in range(strips[c]):
            x_copy(c, s).wait_send()

    def settle_line(c):
        p = order[c]

        def sent(up):
            for s in range(strips[c]):
                z_copy(c, s, up).wait_send()

        @pl.when(place == p)
        def _():
            for s in range(strips[c]):
                done_copy(c, s).wait()

        if p > 0:
            pl.when(place < p)(functools.partial(sent, True))
        if p < top:
            pl.when(place > p)(functools.partial(sent, False))

    def synth(c):
        pert_copy(c).wait()
        if c > 0:
            settle_grid(c - 1)
        if c > 1:
            settle_pair(c - 2)
        for s in range(subs):
            for d in range(grid_count - 1):
                back_copy(c, s, d).wait_recv()
        field = result_v[c].reshape(cols, points)
        wide = 256 if lon_count % 256 == 0 else lon_count
        for left in range(0, lon_count, wide):
            cut = slice(left, left + wide)
            both = [None, None]
            for k in range(mem_dev):
                values = lax.dot_general(
                    field[:, 2 * k * lat_dev : 2 * (k + 1) * lat_dev], table_v[:, cut],
                    (((0,), (0,)), ((), ())), preferred_element_type=jnp.float32,
                )
                for i in range(2):
                    term = values[i * lat_dev : (i + 1) * lat_dev] * pert_v[c, k, i, :, cut].astype(jnp.float32)
                    both[i] = term if k == 0 else both[i] + term
            give_v[c, :, cut] = jnp.where(side == 0, both[1], both[0]).astype(jnp.bfloat16)
            keep_v[c, :, cut] = jnp.where(side == 0, both[0], both[1])
        for s in range(strips[c]):
            x_copy(c, s).start()
        if c == top:
            settle_grid(c)

    def gather(c, s, z):
        p = order[c]
        x_copy(c, s).wait_recv()
        total = keep_v[c, rows(c, s)] + got_v[c, rows(c, s)].astype(jnp.float32)
        for way in range(2):
            up = way == 0
            if (0 < z <= p) if up else (p <= z < top):
                z_copy(c, s, up).wait_recv()
                total = total + come_v[c, way, rows(c, s)].astype(jnp.float32)
        if z == p:
            done_v[rows(c, s)] = total
            done_copy(c, s).start()
        else:
            pass_v[c, rows(c, s)] = total.astype(jnp.bfloat16)
            z_copy(c, s, z < p).start()

    steps = []
    for c in range(chunks):
        p = order[c]
        begin = 12.8 * c
        steps += [(8.4 + begin + 2.2 * s, legendre, (c, s)) for s in range(subs)]
        steps.append((19.1 + begin, synth, (c,)))
        if c > 0:
            steps.append((3.0 + 6.3 * c, spectra, (c,)))
        for z in range(chunks):
            hops = z if z < p else top - z if z > p else max(p, top - p)
            slack = [0.0, 0.5, 1.5][min(top - c, 2)]
            for s in range(strips[c]):
                wire = 12.7 / strips[c]
                ready = 23.0 + slack + begin + wire * (s + 1) + hops * (2.8 + slack + wire)
                steps.append((ready, gather, (c, s, z)))
        if c < top:
            last = max(step[0] for step in steps if step[1] is gather and step[2][0] == c)
            steps.append((last + 3.0, settle_line, (c,)))
    steps.append((26.0 + 12.8 * top, settle_pair, (top - 1,)))
    steps.sort(key=lambda step: step[0])

    spectra(0)
    local(response_ref, weight_v, table_sem.at[1]).wait()
    wave = lax.broadcasted_iota(jnp.int32, weight_v.shape, 0) + g * keep_dev
    weight_v[...] = weight_v[...] * jnp.where(wave == 0, 1.0, 2.0).astype(jnp.float32)
    need = grid_count + (place < top).astype(jnp.int32) + (place > 0).astype(jnp.int32)
    pl.semaphore_wait(barrier, need)
    send_out(0)
    steps = [step for step in steps if step[1] is spectra and step[2] == (1,)] + [
        step for step in steps if not (step[1] is spectra and step[2] == (1,))
    ]
    for _, act, which in steps:
        if act is gather:
            pl.when(place == which[2])(functools.partial(gather, *which))
        else:
            act(*which)
    settle_pair(top)
    settle_line(top)


def whole(alpha, perturbation, legendre, response, table):
    mem_dev, levels, lat_dev, lon_count = alpha.shape
    keep_dev, degrees, lat_count = legendre.shape
    cols = table.shape[0]
    grid_count = cols // (2 * keep_dev)
    chunks = levels // 2
    points = mem_dev * 2 * lat_dev
    waves = 16
    subs = keep_dev // waves
    strips = [4] * (chunks - 1) + [6]
    most = max(strips)
    order = list(range(1, chunks, 2)) + list(range(0, chunks, 2))
    half, wide = jnp.bfloat16, jnp.float32
    field = (mem_dev, 2, lat_dev, lon_count)
    waved = pltpu.VMEM((chunks, grid_count, 2, keep_dev, points), half)
    turned = pltpu.VMEM((grid_count, 2, points // 128 * waves, 128), wide)
    level = (chunks, lat_dev, lon_count)
    dma = pltpu.SemaphoreType.DMA
    peers = grid_count - 1
    return pl.pallas_call(
        functools.partial(whole_kernel, order, waves, strips),
        out_shape=jax.ShapeDtypeStruct((1, lat_dev, lon_count), wide),
        in_specs=[
            pl.BlockSpec(memory_space=pl.ANY),
            pl.BlockSpec(memory_space=pl.ANY),
            pl.BlockSpec(memory_space=pl.ANY),
            pl.BlockSpec(memory_space=pl.ANY),
            pl.BlockSpec(memory_space=pl.ANY),
        ],
        out_specs=pl.BlockSpec(memory_space=pl.ANY),
        scratch_shapes=[
            pltpu.VMEM((cols, lon_count), half), pltpu.VMEM((2,) + field, half), pltpu.VMEM((chunks,) + field, half),
            pltpu.VMEM((keep_dev, degrees, lat_count), half), pltpu.VMEM((keep_dev, degrees), wide),
            waved, waved, waved, waved, turned, turned,
            pltpu.VMEM(level, half), pltpu.VMEM(level, half), pltpu.VMEM(level, wide), pltpu.VMEM(level, half),
            pltpu.VMEM((chunks, 2, lat_dev, lon_count), half), pltpu.VMEM((lat_dev, lon_count), wide),
            dma((2,)), dma((mem_dev,)), dma((subs,)), dma((chunks,)), dma((chunks,)),
            dma((chunks, subs, peers)), dma((chunks, subs, peers)), dma((chunks, subs, peers)), dma((chunks, subs, peers)),
            dma((chunks, most)), dma((chunks, most)), dma((chunks, 2, most)), dma((chunks, 2, most)),
            dma((most,)),
        ],
        compiler_params=pltpu.CompilerParams(
            vmem_limit_bytes=53 * 2**20, collective_id=0, has_side_effects=True
        ),
        cost_estimate=pl.CostEstimate(
            flops=2**35, bytes_accessed=2 * alpha.size, transcendentals=0
        ),
    )(alpha, perturbation, legendre, response, table)


def body(alpha, perturbation, legendre, response):
    mem_dev, levels, lat_dev, lon_count = alpha.shape
    keep_dev = legendre.shape[0]
    grid_count = lax.axis_size("grid")
    members = mem_dev * lax.axis_size("mem")
    cols = 2 * keep_dev
    table = build_table(lon_count, keep_dev, grid_count)
    scale = jnp.float32(1.0 / (lon_count * math.sqrt(members - 1)))
    if keep_dev % 16 == 0 and lat_dev % 128 == 64 and levels == lax.axis_size("mem") and levels in (4, 6, 8):
        return whole(alpha, perturbation, legendre, response, table) * scale

    wave = lax.axis_index("grid") * keep_dev + jnp.arange(keep_dev)
    response = response * jnp.where(wave == 0, 1.0, 2.0).astype(jnp.float32)[:, None]

    points = mem_dev * levels * lat_dev
    lane = math.gcd(points, 128)
    spectra = jnp.einsum("cx,klyx->ckly", table, alpha, preferred_element_type=jnp.float32)
    spectra = spectra.astype(jnp.bfloat16).reshape(grid_count, cols, points // lane, lane)
    spectra = lax.all_to_all(spectra, "grid", split_axis=0, concat_axis=0, tiled=True)
    split = spectra.reshape(grid_count, 2, keep_dev, mem_dev, levels, lat_dev)
    split = jnp.transpose(split, (1, 2, 3, 4, 0, 5)).reshape(2, keep_dev, mem_dev, levels, -1)
    filtered = legendre_filter(split, legendre, response)
    filtered = filtered.reshape(2, keep_dev, mem_dev, levels, grid_count, lat_dev)
    filtered = jnp.transpose(filtered, (4, 0, 1, 2, 3, 5)).reshape(grid_count, cols, points // lane, lane)
    filtered = lax.all_to_all(filtered, "grid", split_axis=0, concat_axis=0, tiled=True)
    filtered = filtered.reshape(grid_count * cols, mem_dev, levels, lat_dev)
    filtered = jnp.transpose(filtered, (1, 2, 3, 0))

    def partial(level, count):
        field = lax.dynamic_slice_in_dim(filtered, level, count, 1)
        weight = lax.dynamic_slice_in_dim(perturbation, level, count, 1)
        values = jnp.einsum("klyc,cx->klyx", field, table, preferred_element_type=jnp.float32)
        return jnp.sum(values * weight, axis=0)

    total = reduce_levels(partial, levels)
    return total * scale


def solution(mesh):
    placed = (
        P("mem", None, "grid", None),
        P("mem", None, "grid", None),
        P("grid", None, None),
        P("grid", None),
    )
    return jax.shard_map(
        body, mesh=mesh, in_specs=placed, out_specs=P("mem", "grid", None), check_vma=False
    )
```
